256 devices in a mesh: py: 8 (over x, y_lo), px: 32 (over y_hi, z, core).
Axes of the slice: x: 4, y: 4 (y_hi: 2, y_lo: 2; y = y_hi * 2 + y_lo), z: 8, core: 2. Of those that a mesh axis runs over, the one named last changes fastest.
Arguments:
- movie: bfloat16 [512, 512, 2048], P('py', 'px'), may hold values from -6 to 6
- traces: bfloat16 [4096, 2048], P('py', 'px'), may hold values from -0.125 to 0.125
- footprints: float32 [512, 512, 512], P('py', 'px'), may hold values from 0 to 1
- block_ids: int32 [8, 32, 4], P('py', 'px'), may hold values from 0 to 32, as said below
Outputs:
- updated: float32 [512, 512, 512], P('py', 'px')
The draws below stay inside these ranges and needn't reach their ends.
Inputs may be any that keep to these rules, and one draw needn't show every extreme that they name: `block_ids`: in each tile's list of 4 entries the live entries come first and are distinct block numbers below 32; the remaining entries equal 32 and mark empty slots. Every tile has at least one live entry, and some tile has all 4 live.
All inputs are finite; a program needn't handle non-finite values.
Results may differ from the reference program's by a relative error of at most 0.0003.
Values may be sent and summed in bfloat16 or wider, within the bound.
No kernel may reach another device: no remote copies, remote signals or barrier semaphores. Data moves between devices by JAX's collectives and lax.ppermute only.
A program may use at most 64 MiB of HBM per device.

```python
import jax
import jax.numpy as jnp
from jax import lax

K = 4096
BLK = 128
SLOTS = 4
ITERS = 2
FRAMES = 2048
ROWS_DEV = 64
COLS_DEV = 16
NBLK = 32
NR = 512
NC = 512
TROWS = 8
TCOLS = 32
N_PY = 8
N_PX = 32


def draw_block_ids(key, part):
    base = jax.random.fold_in(key, 11)
    key_score, key_count, key_full = jax.random.split(base, 3)
    tiles = TROWS * TCOLS
    scores = jax.random.randint(key_score, (tiles, NBLK), 0, 2 ** 20) * NBLK + jnp.arange(NBLK, dtype=jnp.int32)[None, :]
    order = jnp.argsort(scores, axis=1)[:, :SLOTS].astype(jnp.int32)
    counts = jax.random.randint(key_count, (tiles,), 1, SLOTS + 1)
    fullest = jax.random.randint(key_full, (), 0, tiles)
    counts = jnp.where(jnp.arange(tiles) == fullest, SLOTS, counts)
    slot_index = jnp.arange(SLOTS, dtype=jnp.int32)[None, :]
    chosen = jnp.where(slot_index < counts[:, None], order, NBLK)
    return chosen.reshape(TROWS, TCOLS, SLOTS).astype(jnp.int32)


def shard_levels(stream_key, dims, shards, smallest, largest):
    level = 1.0
    for dim, blocks in shards:
        draws = jax.random.uniform(jax.random.fold_in(jax.random.fold_in(stream_key, 6), dim), (blocks,), jnp.float32, smallest / len(shards), largest / len(shards))
        level = level * jnp.repeat(jnp.exp(draws), dims[dim] // blocks).reshape((-1,) + (1,) * (len(dims) - 1 - dim))
    return level


def bell_draw(rng, shape, spread, reach, cuts=(), kind=jnp.bfloat16):
    drawn = jax.random.normal(rng, shape, jnp.float32) * spread
    if len(cuts) > 0:
        drawn = shard_levels(rng, shape, cuts, -0.22, 0.18) * drawn
    return jnp.clip(drawn, min=-reach, max=reach).astype(kind)


def setup_inputs(seed: int = 0) -> dict:
    arg_keys = jax.random.split(jax.random.key(seed), 5)
    return {
        "movie": bell_draw(arg_keys[0], (NR, NC, FRAMES), 1.0, 6.0, ((0, 8), (1, 32))),
        "traces": bell_draw(arg_keys[1], (K, FRAMES), FRAMES ** -0.5, 0.125, ((0, 8), (1, 32))),
        "footprints": jnp.clip(1.0 * jax.random.uniform(arg_keys[2], (NR, NC, SLOTS * BLK), jnp.float32) ** shard_levels(arg_keys[2], (NR, NC, SLOTS * BLK), ((0, 8), (1, 32)), -0.2, 0.2), 0.0, 1.0),
        "block_ids": draw_block_ids(jax.random.fold_in(arg_keys[4], 71), 0),
    }


def reference(movie, traces, footprints, block_ids):
    tiles = N_PY * N_PX
    pix = ROWS_DEV * COLS_DEV
    width = SLOTS * BLK
    nblk = K // BLK
    ytiles = movie.reshape(N_PY, ROWS_DEV, N_PX, COLS_DEV, FRAMES).transpose(0, 2, 1, 3, 4).reshape(tiles, pix, FRAMES)
    atiles = footprints.reshape(N_PY, ROWS_DEV, N_PX, COLS_DEV, width).transpose(0, 2, 1, 3, 4).reshape(tiles, pix, width)
    ids = block_ids.reshape(tiles, SLOTS)
    onehot = (ids[:, :, None] == jnp.arange(nblk, dtype=jnp.int32)[None, None, :]).astype(jnp.float32)
    live = lax.optimization_barrier(jnp.sum(onehot, axis=2))
    blocks = traces.reshape(nblk, BLK, FRAMES).astype(jnp.float32)
    gram_all = jnp.dot(traces, traces.T, preferred_element_type=jnp.float32).reshape(nblk, BLK, nblk, BLK)

    def per_tile(args):
        tile_movie, hot = args
        picked = jnp.einsum('sb,bnf->snf', hot, blocks).astype(jnp.bfloat16).reshape(width, FRAMES)
        cross = jnp.dot(tile_movie, picked.T, preferred_element_type=jnp.float32)
        gram = jnp.einsum('sb,bncq,dc->sndq', hot, gram_all, hot, precision=lax.Precision.HIGHEST).reshape(width, width)
        return (cross, gram)
    cross, gram = lax.map(per_tile, (ytiles, onehot))
    column_live = jnp.repeat(live, BLK, axis=1)
    denom = jnp.diagonal(gram, axis1=1, axis2=2) + 1e-06 + (1.0 - column_live)
    current = atiles * column_live[:, None, :]
    pixall = NR * NC
    for step in range(ITERS):
        for slot in range(SLOTS):
            low = slot * BLK
            columns = gram[:, :, low:low + BLK]
            resid = cross[:, :, low:low + BLK] - jnp.einsum('tpk,tkn->tpn', current, columns, precision=lax.Precision.HIGHEST)
            fresh = jnp.maximum(current[:, :, low:low + BLK] + resid / denom[:, None, low:low + BLK], 0.0)
            current = current.at[:, :, low:low + BLK].set(fresh)
        colsq = lax.optimization_barrier(jnp.sum(current * current, axis=1)).reshape(tiles, SLOTS, BLK)
        totals = jnp.einsum('tsb,tsn->bn', onehot, colsq, precision=lax.Precision.HIGHEST)
        factor = 1.0 / jnp.sqrt(totals / pixall + 1e-06)
        scale = jnp.einsum('tsb,bn->tsn', onehot, factor, precision=lax.Precision.HIGHEST).reshape(tiles, width)
        current = current * scale[:, None, :]
    return current.reshape(N_PY, N_PX, ROWS_DEV, COLS_DEV, width).transpose(0, 2, 1, 3, 4).reshape(NR, NC, width)
```

```python
import jax
import jax.numpy as jnp
from jax import lax
from jax.experimental import pallas as pl
from jax.experimental.pallas import tpu as pltpu
from jax.sharding import Mesh
from jax.sharding import PartitionSpec as P

BLK = 128
SLOTS = 4
WIDTH = SLOTS * BLK
NBLK = 32
ITERS = 2
PY = ("py_0", "py_1")
PX = ("px_0", "px_1", "px_2")
EVERY = ("py_0", "py_1", "px_0", "px_1", "px_2")
COLUMN = ("py_0", "py_1", "px_1")
PLANE = ("py_0", "py_1", "px_0", "px_2")
CORE_MATES = ("py_0", "py_1", "px_0", "px_1")
CORE = "px_2"


def to_everyone(value, axes):
    copies = jnp.broadcast_to(value[None], (lax.axis_size(axes), *value.shape))
    return lax.all_to_all(copies, axes, split_axis=0, concat_axis=0, tiled=True)


def select_kernel(place_ref, ids_ref, rows_ref, out_ref):
    tiles = out_ref.shape[0]

    @pl.loop(0, tiles)
    def _(tile):
        for slot in range(SLOTS):
            block = ids_ref[tile ^ place_ref[0, 0], slot]
            live = block < NBLK
            safe = jnp.where(live, block, 0)
            group = safe // SLOTS
            lane = pl.multiple_of((safe % SLOTS) * BLK, BLK)

            @pl.when(live)
            def _():
                out_ref[tile, :, :, slot * BLK : (slot + 1) * BLK] = rows_ref[
                    group, :, :, pl.ds(lane, BLK)
                ]

            @pl.when(jnp.logical_not(live))
            def _():
                out_ref[tile, :, :, slot * BLK : (slot + 1) * BLK] = jnp.zeros(
                    (rows_ref.shape[1], 8, BLK), out_ref.dtype
                )


def select(place, tile_ids, rows):
    tiles = tile_ids.shape[0]
    return pl.pallas_call(
        select_kernel,
        out_shape=jax.ShapeDtypeStruct((tiles, *rows.shape[1:]), rows.dtype),
        in_specs=[
            pl.BlockSpec(memory_space=pltpu.SMEM),
            pl.BlockSpec(memory_space=pltpu.SMEM),
            pl.BlockSpec(memory_space=pltpu.VMEM),
        ],
        out_specs=pl.BlockSpec(memory_space=pltpu.VMEM),
        cost_estimate=pl.CostEstimate(flops=1 << 20, bytes_accessed=1 << 22, transcendentals=0),
        name="select",
    )(place, tile_ids, rows)


def totals_of(colsq, mate_ids, my_ids, peer_ids):
    seen = to_everyone(colsq, CORE_MATES).reshape(-1, BLK)
    wanted = jnp.concatenate([my_ids, peer_ids])
    match = (wanted[:, None] == mate_ids.reshape(1, -1)).astype(jnp.float32)
    sums = jnp.dot(match, seen, precision=lax.Precision.HIGHEST)
    other = lax.ppermute(sums[SLOTS:], CORE, [(0, 1), (1, 0)])
    return sums[:SLOTS] + other


def swapped(value, axis, bit):
    size = lax.axis_size(axis)
    return lax.ppermute(value, axis, [(i, i ^ bit) for i in range(size)])


def doubled(ids, axis):
    bit = 1
    while bit < lax.axis_size(axis):
        ids = jnp.concatenate([ids, swapped(ids, axis, bit)])
        bit *= 2
    return ids


def in_place_order(value, dim, axis):
    size = value.shape[dim]
    at = lax.axis_index(axis)
    bit = 1
    while bit < size:
        shape = (*value.shape[:dim], size // (2 * bit), 2, bit, *value.shape[dim + 1 :])
        flipped = jnp.flip(value.reshape(shape), dim + 1).reshape(value.shape)
        value = jnp.where((at & bit) != 0, flipped, value)
        bit *= 2
    return value


def per_device(movie, traces, footprints, block_ids):
    rows, cols, frames = movie.shape
    pixels = rows * cols
    n_group = lax.axis_size(PY)
    n_z = lax.axis_size("px_1")
    sizes = tuple(lax.axis_size(a) for a in EVERY)
    part = traces.shape[1] // n_group
    my_ids = block_ids.reshape(SLOTS)
    pieces = traces.T.reshape(n_group, 1, part, traces.shape[0])
    pieces = jnp.broadcast_to(pieces, (n_group, n_z, part, traces.shape[0]))
    pieces = pieces.reshape(n_group * n_z, part, traces.shape[0])
    spread = lax.all_to_all(pieces, COLUMN, split_axis=0, concat_axis=0, tiled=True)
    plane_ids = my_ids[None]
    for axis in reversed(PLANE):
        plane_ids = doubled(plane_ids, axis)
    every_ids = doubled(plane_ids, "px_1")
    peer_ids = plane_ids[1]
    mate_ids = every_ids.reshape(n_z, *sizes[:3], sizes[4], SLOTS)[:, :, :, :, 0]
    mate_ids = mate_ids.transpose(1, 2, 3, 0, 4)
    for dim, axis in enumerate(CORE_MATES):
        mate_ids = in_place_order(mate_ids, dim, axis)
    place = lax.axis_index(PLANE).reshape(1, 1)

    outgoing = select(place, plane_ids, spread.reshape(n_group, n_z, part, traces.shape[0]))
    received = lax.all_to_all(outgoing, PLANE, split_axis=0, concat_axis=0, tiled=True)
    picked = received.reshape(n_group, sizes[2], sizes[4], n_z, part, WIDTH)
    picked = picked.transpose(1, 3, 2, 0, 4, 5).reshape(frames, WIDTH)

    tile_movie = movie.reshape(pixels, frames)
    cross = lax.dot_general(
        tile_movie, picked, (((1,), (0,)), ((), ())), preferred_element_type=jnp.float32
    )
    gram = lax.dot_general(
        picked, picked, (((0,), (0,)), ((), ())), preferred_element_type=jnp.float32
    )
    live = (my_ids < NBLK).astype(jnp.float32)
    column_live = jnp.repeat(live, BLK)
    wide = picked.astype(jnp.float32)
    denom = jnp.sum(wide * wide, axis=0) + 1e-06 + (1.0 - column_live)
    current = footprints.reshape(pixels, WIDTH) * column_live[None, :]
    pixall = pixels * lax.axis_size(EVERY)
    for step in range(ITERS):
        for slot in range(SLOTS):
            low = slot * BLK
            resid = cross[:, low : low + BLK] - jnp.dot(
                current, gram[:, low : low + BLK], precision=lax.Precision.HIGHEST
            )
            fresh = jnp.maximum(
                current[:, low : low + BLK] + resid / denom[None, low : low + BLK], 0.0
            )
            current = current.at[:, low : low + BLK].set(fresh)
        colsq = jnp.sum(current * current, axis=0).reshape(SLOTS, BLK)
        totals = totals_of(colsq, mate_ids, my_ids, peer_ids)
        scale = live[:, None] / jnp.sqrt(totals / pixall + 1e-06)
        current = current * scale.reshape(1, WIDTH)
    return current.reshape(rows, cols, WIDTH)


def solution(mesh):
    finer = Mesh(mesh.devices.reshape(4, 2, 2, 8, 2), EVERY)
    placed = (P(PY, PX, None), P(PY, PX), P(PY, PX, None), P(PY, PX, None))
    return jax.shard_map(
        per_device, mesh=finer, in_specs=placed, out_specs=P(PY, PX, None), check_vma=False
    )
```

```python
import jax
import jax.numpy as jnp
from jax import lax
from jax.experimental import pallas as pl
from jax.experimental.pallas import tpu as pltpu
from jax.sharding import Mesh
from jax.sharding import PartitionSpec as P


BLK = 128
SLOTS = 4
WIDTH = SLOTS * BLK
NBLK = 32
EVERY = ("py_0", "py_1", "px_0", "px_1", "px_2")
PY = ("py_0", "py_1")
PX = ("px_0", "px_1", "px_2")
COLUMN = ("py_0", "py_1", "px_1")
PLANE = ("py_0", "py_1", "px_2", "px_0")
MATES = ("px_0", "py_1", "px_1", "py_0")
CORE = "px_2"
F32 = jnp.float32
BF16 = jnp.bfloat16
ROW_TILE = 512
VMEM_BYTES = 48 << 20


def to_everyone(value, axes):
    copies = jnp.broadcast_to(value[None], (lax.axis_size(axes), *value.shape))
    return lax.all_to_all(copies, axes, split_axis=0, concat_axis=0, tiled=True)


def swapped(value, axis, bits):
    return lax.ppermute(value, axis, [(i, i ^ bits) for i in range(lax.axis_size(axis))])


def in_place_order(value, dim, axis):
    size = value.shape[dim]
    at = lax.axis_index(axis)
    bit = 1
    while bit < size:
        shape = (*value.shape[:dim], size // (2 * bit), 2, bit, *value.shape[dim + 1 :])
        flipped = jnp.flip(value.reshape(shape), dim + 1).reshape(value.shape)
        value = jnp.where((at & bit) != 0, flipped, value)
        bit *= 2
    return value


def select_kernel(place_ref, *refs):
    *ids_refs, rows_ref, out_hbm, zero_ref, sem = refs
    zero_ref[...] = jnp.zeros_like(zero_ref)
    place = place_ref[0, 0]
    chunk = ids_refs[0].shape[0]
    for far, ids_ref in enumerate(ids_refs):

        @pl.loop(0, chunk)
        def _(near):
            tile = (far * chunk + near) ^ place
            for slot in range(SLOTS):
                block = ids_ref[near, slot]
                target = out_hbm.at[tile, slot]

                @pl.when(block < NBLK)
                def _():
                    lane = pl.multiple_of((block % SLOTS) * BLK, BLK)
                    source = rows_ref.at[block // SLOTS, :, :, pl.ds(lane, BLK)]
                    pltpu.make_async_copy(source, target, sem).start()

                @pl.when(block >= NBLK)
                def _():
                    pltpu.make_async_copy(zero_ref, target, sem).start()

    pltpu.make_async_copy(out_hbm, out_hbm, sem).wait()


def select(place, ids_pieces, rows):
    tiles = sum(piece.shape[0] for piece in ids_pieces)
    smem = pl.BlockSpec(memory_space=pltpu.SMEM)
    anywhere = pl.BlockSpec(memory_space=pltpu.HBM)
    return pl.pallas_call(
        select_kernel,
        out_shape=jax.ShapeDtypeStruct((tiles, SLOTS, *rows.shape[1:3], BLK), rows.dtype),
        in_specs=[smem] * (1 + len(ids_pieces)) + [pl.BlockSpec(memory_space=pltpu.VMEM)],
        out_specs=anywhere,
        scratch_shapes=[
            pltpu.VMEM((rows.shape[1], rows.shape[2], BLK), rows.dtype),
            pltpu.SemaphoreType.DMA,
        ],
        cost_estimate=pl.CostEstimate(flops=1 << 20, bytes_accessed=1 << 22, transcendentals=0),
        name="select",
    )(place, *ids_pieces, rows)


def sweep(a_ref, hi_ref, lo_ref, cross_ref, gram_ref, inv_ref, colsq_ref):
    pixels = a_ref.shape[0]
    for slot in range(SLOTS):
        c = slice(slot * BLK, (slot + 1) * BLK)
        weights = gram_ref[slot]
        total = jnp.zeros((1, BLK), F32)
        for low in range(0, pixels, ROW_TILE):
            r = slice(low, low + ROW_TILE)
            both = jnp.dot(hi_ref[r, :], weights, preferred_element_type=F32)
            both += jnp.dot(lo_ref[r, :], weights, preferred_element_type=F32)
            resid = cross_ref[r, c] - (both[:, :BLK] + both[:, BLK:])
            fresh = jnp.maximum(a_ref[r, c] + resid * inv_ref[:, c], 0.0)
            a_ref[r, c] = fresh
            if slot < SLOTS - 1:
                high = fresh.astype(BF16)
                hi_ref[r, c] = high
                lo_ref[r, c] = (fresh - high.astype(F32)).astype(BF16)
            total += jnp.sum(fresh * fresh, axis=0, keepdims=True)
        colsq_ref[slot : slot + 1, :] = total


def put_parts(value, r, a_ref, hi_ref, lo_ref):
    a_ref[r, :] = value
    high = value.astype(BF16)
    hi_ref[r, :] = high
    lo_ref[r, :] = (value - high.astype(F32)).astype(BF16)


def first_kernel(
    live_ref, recv_ref, movie_hbm, foot_hbm,
    a_ref, colsq_ref, cross_ref, gram_ref, inv_ref,
    movie_ref, foot_ref, picked_ref, square_ref, hi_ref, lo_ref, sems,
):
    copies = [
        pltpu.make_async_copy(source, target, sems.at[i])
        for i, (source, target) in enumerate(
            ((movie_hbm, movie_ref), (foot_hbm, foot_ref))
        )
    ]
    for copy in copies:
        copy.start()
    groups, cores, halves, _, depth, part, _ = recv_ref.shape
    base = 0
    for half in range(halves):
        for z in range(depth):
            for core in range(cores):
                size = groups * part
                for slot in range(SLOTS):
                    piece = recv_ref[:, core, half, slot, z].astype(F32).reshape(size, BLK)
                    picked_ref[base : base + size, slot * BLK : (slot + 1) * BLK] = piece.astype(BF16)
                base += size
    picked = picked_ref[...]
    square_ref[...] = lax.dot_general(
        picked, picked, (((0,), (0,)), ((), ())), preferred_element_type=F32
    )
    eye = lax.broadcasted_iota(jnp.int32, (BLK, BLK), 0) == lax.broadcasted_iota(
        jnp.int32, (BLK, BLK), 1
    )
    for slot in range(SLOTS):
        c = slice(slot * BLK, (slot + 1) * BLK)
        columns = square_ref[:, c]
        high = columns.astype(BF16)
        gram_ref[slot, :, :BLK] = high
        gram_ref[slot, :, BLK:] = (columns - high.astype(F32)).astype(BF16)
        diagonal = jnp.sum(jnp.where(eye, square_ref[c, c], 0.0), axis=0, keepdims=True)
        inv_ref[:, c] = 1.0 / (diagonal + 1e-06 + (1.0 - live_ref[:, c]))
    copies[0].wait()
    pixels = movie_ref.shape[0]
    for low in range(0, pixels, ROW_TILE):
        r = slice(low, low + ROW_TILE)
        cross_ref[r, :] = jnp.dot(movie_ref[r, :], picked, preferred_element_type=F32)
    copies[1].wait()
    for low in range(0, pixels, ROW_TILE):
        r = slice(low, low + ROW_TILE)
        put_parts(foot_ref[r, :] * live_ref[...], r, a_ref, hi_ref, lo_ref)
    sweep(a_ref, hi_ref, lo_ref, cross_ref, gram_ref, inv_ref, colsq_ref)


def second_kernel(
    scale_ref, old_ref, cross_ref, gram_ref, inv_ref, a_ref, colsq_ref, hi_ref, lo_ref
):
    for low in range(0, old_ref.shape[0], ROW_TILE):
        r = slice(low, low + ROW_TILE)
        put_parts(old_ref[r, :] * scale_ref[...], r, a_ref, hi_ref, lo_ref)
    sweep(a_ref, hi_ref, lo_ref, cross_ref, gram_ref, inv_ref, colsq_ref)


def first_pass(live, received, tile_movie, tile_foot):
    pixels, frames = tile_movie.shape
    vmem = pl.BlockSpec(memory_space=pltpu.VMEM)
    hbm = pl.BlockSpec(memory_space=pltpu.HBM)
    return pl.pallas_call(
        first_kernel,
        out_shape=(
            pltpu.VMEM((pixels, WIDTH), F32),
            pltpu.VMEM((SLOTS, BLK), F32),
            pltpu.VMEM((pixels, WIDTH), F32),
            pltpu.VMEM((SLOTS, WIDTH, 2 * BLK), BF16),
            pltpu.VMEM((1, WIDTH), F32),
        ),
        in_specs=[vmem, vmem, hbm, hbm],
        out_specs=(vmem,) * 5,
        scratch_shapes=[
            pltpu.VMEM(tile_movie.shape, tile_movie.dtype),
            pltpu.VMEM(tile_foot.shape, F32),
            pltpu.VMEM((frames, WIDTH), BF16),
            pltpu.VMEM((WIDTH, WIDTH), F32),
            pltpu.VMEM((pixels, WIDTH), BF16),
            pltpu.VMEM((pixels, WIDTH), BF16),
            pltpu.SemaphoreType.DMA((2,)),
        ],
        compiler_params=pltpu.CompilerParams(vmem_limit_bytes=VMEM_BYTES),
        cost_estimate=pl.CostEstimate(flops=7 << 30, bytes_accessed=12 << 20, transcendentals=0),
        name="first_pass",
    )(live, received, tile_movie, tile_foot)


def second_pass(scale, a, cross, gram, inv):
    pixels = a.shape[0]
    vmem = pl.BlockSpec(memory_space=pltpu.VMEM)
    return pl.pallas_call(
        second_kernel,
        out_shape=(pltpu.VMEM((pixels, WIDTH), F32), pltpu.VMEM((SLOTS, BLK), F32)),
        in_specs=[vmem] * 5,
        out_specs=(vmem,) * 2,
        scratch_shapes=[pltpu.VMEM((pixels, WIDTH), BF16), pltpu.VMEM((pixels, WIDTH), BF16)],
        compiler_params=pltpu.CompilerParams(vmem_limit_bytes=VMEM_BYTES // 2),
        cost_estimate=pl.CostEstimate(flops=4 << 30, bytes_accessed=8 << 20, transcendentals=0),
        name="second_pass",
    )(scale, a, cross, gram, inv)


def totals_of(colsq, match):
    seen = to_everyone(colsq, MATES).reshape(-1, BLK)
    sums = jnp.dot(match, seen, precision=lax.Precision.HIGHEST)
    return sums[:SLOTS] + swapped(sums[SLOTS:], CORE, 1)


def per_device(movie, traces, footprints, block_ids):
    rows, cols, frames = movie.shape
    pixels = rows * cols
    n_group = lax.axis_size(PY)
    n_z = lax.axis_size("px_1")
    sizes = {axis: lax.axis_size(axis) for axis in EVERY}
    part = traces.shape[1] // n_group
    my_ids = block_ids.reshape(SLOTS)

    pieces = traces.T.reshape(n_group, 1, part, traces.shape[0])
    pieces = jnp.broadcast_to(pieces, (n_group, n_z, part, traces.shape[0]))
    pieces = pieces.reshape(n_group * n_z, part, traces.shape[0])
    spread = lax.all_to_all(pieces, COLUMN, split_axis=0, concat_axis=0, tiled=True)
    spread = spread.reshape(n_group, n_z, part, traces.shape[0])
    spread = pltpu.with_memory_space_constraint(spread, pltpu.VMEM)

    other_half = swapped(my_ids[None], "px_0", 1)
    near = jnp.concatenate([my_ids[None], other_half])
    near = jnp.concatenate([near] + [swapped(near, ("py_1", CORE), bits) for bits in (1, 2, 3)])
    plane_ids = [near] + [swapped(near, "py_0", bits) for bits in (1, 2, 3)]
    place = lax.axis_index(PLANE).reshape(1, 1)
    outgoing = select(place, plane_ids, spread)
    outgoing, every_ids = lax.optimization_barrier((outgoing, jnp.concatenate(plane_ids)))
    received = lax.all_to_all(outgoing, PLANE, split_axis=0, concat_axis=0, tiled=True)
    received = received.reshape(n_group, sizes[CORE], sizes["px_0"], SLOTS, n_z, part, BLK)
    received = pltpu.with_memory_space_constraint(received, pltpu.VMEM)
    for bit in (1, 2, 4):
        far = swapped(every_ids, "px_1", bit)
        every_ids = jnp.concatenate([every_ids, far])
    mate_ids = every_ids.reshape(n_z, sizes["py_0"], sizes["py_1"], 2, sizes["px_0"], SLOTS)
    mate_ids = mate_ids[:, :, :, 0].transpose(3, 2, 0, 1, 4)
    for dim, axis in enumerate(MATES):
        mate_ids = in_place_order(mate_ids, dim, axis)
    wanted = jnp.concatenate([my_ids, near[2]])
    match = (wanted[:, None] == mate_ids.reshape(1, -1)).astype(F32)
    live = (my_ids < NBLK).astype(F32)
    column_live = jnp.repeat(live, BLK).reshape(1, WIDTH)
    column_live, match = lax.optimization_barrier((column_live, match))

    pixall = pixels * lax.axis_size(EVERY)
    tile_movie = pltpu.with_memory_space_constraint(movie.reshape(pixels, frames), pltpu.HBM)
    tile_foot = pltpu.with_memory_space_constraint(footprints.reshape(pixels, WIDTH), pltpu.HBM)
    current, colsq, cross, gram, inv = first_pass(column_live, received, tile_movie, tile_foot)
    current, cross = (pltpu.with_memory_space_constraint(x, pltpu.VMEM) for x in (current, cross))
    scale = live[:, None] / jnp.sqrt(totals_of(colsq, match) / pixall + 1e-06)
    current, colsq = second_pass(scale.reshape(1, WIDTH), current, cross, gram, inv)
    scale = live[:, None] / jnp.sqrt(totals_of(colsq, match) / pixall + 1e-06)
    return (current * scale.reshape(1, WIDTH)).reshape(rows, cols, WIDTH)


def solution(mesh):
    finer = Mesh(mesh.devices.reshape(4, 2, 2, 8, 2), EVERY)
    placed = (P(PY, PX, None), P(PY, PX), P(PY, PX, None), P(PY, PX, None))

    return jax.shard_map(
        per_device, mesh=finer, in_specs=placed, out_specs=P(PY, PX, None), check_vma=False
    )
```

```python
import jax
import jax.numpy as jnp
from jax import lax
from jax.experimental import pallas as pl
from jax.experimental.pallas import tpu as pltpu
from jax.sharding import Mesh
from jax.sharding import PartitionSpec as P


BLK = 128
SLOTS = 4
WIDTH = SLOTS * BLK
NBLK = 32
EVERY = ("py_0", "py_1", "px_0", "px_1", "px_2")
PY = ("py_0", "py_1")
PX = ("px_0", "px_1", "px_2")
COLUMN = ("py_0", "py_1", "px_1")
PLANE = ("py_0", "py_1", "px_2", "px_0")
MATES = ("px_0", "py_1", "px_1", "py_0")
CORE = "px_2"
F32 = jnp.float32
BF16 = jnp.bfloat16
ROW_TILE = 512
VMEM_BYTES = 24 << 20


def to_everyone(value, axes):
    copies = jnp.broadcast_to(value[None], (lax.axis_size(axes), *value.shape))
    return lax.all_to_all(copies, axes, split_axis=0, concat_axis=0, tiled=True)


def swapped(value, axis, bits):
    return lax.ppermute(value, axis, [(i, i ^ bits) for i in range(lax.axis_size(axis))])


def in_place_order(value, dim, axis):
    size = value.shape[dim]
    at = lax.axis_index(axis)
    bit = 1
    while bit < size:
        shape = (*value.shape[:dim], size // (2 * bit), 2, bit, *value.shape[dim + 1 :])
        flipped = jnp.flip(value.reshape(shape), dim + 1).reshape(value.shape)
        value = jnp.where((at & bit) != 0, flipped, value)
        bit *= 2
    return value


def select_kernel(place_ref, *refs):
    *ids_refs, rows_ref, out_hbm, sem = refs
    place = place_ref[0, 0]
    chunk = ids_refs[0].shape[0]
    depth = rows_ref.shape[0] // (NBLK // SLOTS)
    for far, ids_ref in enumerate(ids_refs):

        @pl.loop(0, chunk, unroll=True)
        def _(near):
            tile = (far * chunk + near) ^ place
            for slot in range(SLOTS):
                block = jnp.minimum(ids_ref[near, slot], NBLK - 1)
                group = pl.multiple_of((block // SLOTS) * depth, depth)
                lane = pl.multiple_of((block % SLOTS) * BLK, BLK)
                pltpu.make_async_copy(
                    rows_ref.at[pl.ds(group, depth), :, pl.ds(lane, BLK)],
                    out_hbm.at[tile, slot],
                    sem,
                ).start()

    pltpu.make_async_copy(out_hbm, out_hbm, sem).wait()


def select(place, ids_pieces, rows):
    depth = rows.shape[0] // (NBLK // SLOTS)
    tiles = sum(piece.shape[0] for piece in ids_pieces)
    smem = pl.BlockSpec(memory_space=pltpu.SMEM)
    anywhere = pl.BlockSpec(memory_space=pltpu.HBM)
    return pl.pallas_call(
        select_kernel,
        out_shape=jax.ShapeDtypeStruct((tiles, SLOTS, depth, rows.shape[1], BLK), rows.dtype),
        in_specs=[smem] * (1 + len(ids_pieces)) + [pl.BlockSpec(memory_space=pltpu.VMEM)],
        out_specs=anywhere,
        scratch_shapes=[
            pltpu.SemaphoreType.DMA,
        ],
        cost_estimate=pl.CostEstimate(flops=1 << 20, bytes_accessed=1 << 22, transcendentals=0),
        compiler_params=pltpu.CompilerParams(vmem_limit_bytes=2 << 20),
        name="select",
    )(place, *ids_pieces, rows)


def sweep(base, a_ref, hi_ref, lo_ref, cross_ref, gram_ref, inv_ref, colsq_ref):
    pixels = a_ref.shape[0]
    for slot in range(SLOTS):
        c = slice(slot * BLK, (slot + 1) * BLK)
        weights = gram_ref[slot]
        total = jnp.zeros((1, BLK), F32)
        for low in range(0, pixels, ROW_TILE):
            r = slice(low, low + ROW_TILE)
            both = jnp.dot(hi_ref[r, :], weights, preferred_element_type=F32)
            both += jnp.dot(lo_ref[r, :], weights, preferred_element_type=F32)
            resid = cross_ref[r, c] - (both[:, :BLK] + both[:, BLK:])
            fresh = jnp.maximum(base(r, c) + resid * inv_ref[:, c], 0.0)
            a_ref[r, c] = fresh
            if slot < SLOTS - 1:
                high = fresh.astype(BF16)
                hi_ref[r, c] = high
                lo_ref[r, c] = (fresh - high.astype(F32)).astype(BF16)
            total += jnp.sum(fresh * fresh, axis=0, keepdims=True)
        colsq_ref[slot : slot + 1, :] = total


def put_parts(value, r, hi_ref, lo_ref):
    high = value.astype(BF16)
    hi_ref[r, :] = high
    lo_ref[r, :] = (value - high.astype(F32)).astype(BF16)


def first_kernel(
    ids_ref, live_ref, recv_ref, movie_hbm, foot_hbm,
    a_ref, colsq_ref, cross_ref, gram_ref, inv_ref,
    movie_ref, foot_ref, picked_ref, square_ref, hi_ref, lo_ref, sems,
):
    pixels = movie_ref.shape[0]
    tiles = [slice(low, low + ROW_TILE) for low in range(0, pixels, ROW_TILE)]
    movies = [
        pltpu.make_async_copy(movie_hbm.at[r, :], movie_ref.at[r, :], sems.at[i])
        for i, r in enumerate(tiles)
    ]
    foots = [
        pltpu.make_async_copy(foot_hbm.at[r, :], foot_ref.at[r, :], sems.at[len(tiles) + i])
        for i, r in enumerate(tiles)
    ]
    for copy in movies + foots:
        copy.start()
    groups, cores, halves, _, depth, part, _ = recv_ref.shape
    size = groups * part
    base = 0
    for half in range(halves):
        for z in range(depth):
            for core in range(cores):
                for slot in range(SLOTS):
                    piece = recv_ref[:, core, half, slot, z].astype(F32).reshape(size, BLK)
                    picked_ref[base : base + size, slot * BLK : (slot + 1) * BLK] = piece.astype(BF16)
                base += size
    for slot in range(SLOTS):

        @pl.when(ids_ref[0, slot] >= NBLK)
        def _():
            picked_ref[:, slot * BLK : (slot + 1) * BLK] = jnp.zeros((picked_ref.shape[0], BLK), BF16)

    picked = picked_ref[...]
    square_ref[...] = lax.dot_general(
        picked, picked, (((0,), (0,)), ((), ())), preferred_element_type=F32
    )
    eye = lax.broadcasted_iota(jnp.int32, (BLK, BLK), 0) == lax.broadcasted_iota(
        jnp.int32, (BLK, BLK), 1
    )
    for slot in range(SLOTS):
        c = slice(slot * BLK, (slot + 1) * BLK)
        columns = square_ref[:, c]
        high = columns.astype(BF16)
        gram_ref[slot, :, :BLK] = high
        gram_ref[slot, :, BLK:] = (columns - high.astype(F32)).astype(BF16)
        diagonal = jnp.sum(jnp.where(eye, square_ref[c, c], 0.0), axis=0, keepdims=True)
        inv_ref[:, c] = 1.0 / (diagonal + 1e-06 + (1.0 - live_ref[:, c]))
    for r, copy in zip(tiles, movies):
        copy.wait()
        cross_ref[r, :] = jnp.dot(movie_ref[r, :], picked, preferred_element_type=F32)
    for r, copy in zip(tiles, foots):
        copy.wait()
        put_parts(foot_ref[r, :] * live_ref[...], r, hi_ref, lo_ref)
    sweep(
        lambda r, c: foot_ref[r, c] * live_ref[:, c],
        a_ref, hi_ref, lo_ref, cross_ref, gram_ref, inv_ref, colsq_ref,
    )


def second_kernel(
    scale_ref, old_ref, cross_ref, gram_ref, inv_ref, a_ref, colsq_ref, hi_ref, lo_ref
):
    for low in range(0, old_ref.shape[0], ROW_TILE):
        r = slice(low, low + ROW_TILE)
        put_parts(old_ref[r, :] * scale_ref[...], r, hi_ref, lo_ref)
    sweep(
        lambda r, c: old_ref[r, c] * scale_ref[:, c],
        a_ref, hi_ref, lo_ref, cross_ref, gram_ref, inv_ref, colsq_ref,
    )


def last_kernel(scale_ref, a_ref, out_hbm, buffer_ref, sems):
    step = buffer_ref.shape[0] // sems.shape[0]
    copies = []
    for i in range(sems.shape[0]):
        r = slice(i * step, (i + 1) * step)
        buffer_ref[r, :] = a_ref[r, :] * scale_ref[...]
        copy = pltpu.make_async_copy(buffer_ref.at[r, :], out_hbm.at[r, :], sems.at[i])
        copy.start()
        copies.append(copy)
    for copy in copies:
        copy.wait()


VMEM_SPEC = pl.BlockSpec(memory_space=pltpu.VMEM)
HBM_SPEC = pl.BlockSpec(memory_space=pltpu.HBM)
SMEM_SPEC = pl.BlockSpec(memory_space=pltpu.SMEM)


def first_pass(ids, live, received, tile_movie, tile_foot):
    pixels, frames = tile_movie.shape
    return pl.pallas_call(
        first_kernel,
        out_shape=(
            pltpu.VMEM((pixels, WIDTH), F32),
            pltpu.VMEM((SLOTS, BLK), F32),
            pltpu.VMEM((pixels, WIDTH), F32),
            pltpu.VMEM((SLOTS, WIDTH, 2 * BLK), BF16),
            pltpu.VMEM((1, WIDTH), F32),
        ),
        in_specs=[SMEM_SPEC] + [VMEM_SPEC] * 2 + [HBM_SPEC] * 2,
        out_specs=(VMEM_SPEC,) * 5,
        scratch_shapes=[
            pltpu.VMEM((pixels, frames), BF16),
            pltpu.VMEM((pixels, WIDTH), F32),
            pltpu.VMEM((frames, WIDTH), BF16),
            pltpu.VMEM((WIDTH, WIDTH), F32),
            pltpu.VMEM((pixels, WIDTH), BF16),
            pltpu.VMEM((pixels, WIDTH), BF16),
            pltpu.SemaphoreType.DMA((2 * pixels // ROW_TILE,)),
        ],
        compiler_params=pltpu.CompilerParams(vmem_limit_bytes=2 * VMEM_BYTES),
        cost_estimate=pl.CostEstimate(flops=7 << 30, bytes_accessed=12 << 20, transcendentals=0),
        name="first_pass",
    )(ids, live, received, tile_movie, tile_foot)


def second_pass(scale, a, cross, gram, inv):
    pixels = a.shape[0]
    return pl.pallas_call(
        second_kernel,
        out_shape=(pltpu.VMEM((pixels, WIDTH), F32), pltpu.VMEM((SLOTS, BLK), F32)),
        in_specs=[VMEM_SPEC] * 5,
        out_specs=(VMEM_SPEC,) * 2,
        scratch_shapes=[pltpu.VMEM((pixels, WIDTH), BF16), pltpu.VMEM((pixels, WIDTH), BF16)],
        compiler_params=pltpu.CompilerParams(vmem_limit_bytes=VMEM_BYTES),
        cost_estimate=pl.CostEstimate(flops=4 << 30, bytes_accessed=8 << 20, transcendentals=0),
        name="second_pass",
    )(scale, a, cross, gram, inv)


def last_scaling(scale, a):
    return pl.pallas_call(
        last_kernel,
        out_shape=jax.ShapeDtypeStruct(a.shape, F32),
        in_specs=[VMEM_SPEC] * 2,
        out_specs=HBM_SPEC,
        scratch_shapes=[pltpu.VMEM(a.shape, F32), pltpu.SemaphoreType.DMA((8,))],
        compiler_params=pltpu.CompilerParams(vmem_limit_bytes=4 << 20),
        name="last_scaling",
    )(scale, a)


def totals_of(colsq, match):
    seen = to_everyone(colsq, MATES).reshape(-1, BLK)
    sums = jnp.dot(match, seen, precision=lax.Precision.HIGHEST)
    return sums[:SLOTS] + swapped(sums[SLOTS:], CORE, 1)


def per_device(movie, traces, footprints, block_ids):
    rows, cols, frames = movie.shape
    pixels = rows * cols
    n_group = lax.axis_size(PY)
    n_z = lax.axis_size("px_1")
    sizes = {axis: lax.axis_size(axis) for axis in EVERY}
    part = traces.shape[1] // n_group
    my_ids = block_ids.reshape(SLOTS)

    pieces = traces.T.reshape(n_group, 1, part, traces.shape[0])
    pieces = jnp.broadcast_to(pieces, (n_group, n_z, part, traces.shape[0]))
    pieces = pieces.reshape(n_group * n_z, part, traces.shape[0])
    pieces = pltpu.with_memory_space_constraint(pieces, pltpu.VMEM)
    spread = lax.all_to_all(pieces, COLUMN, split_axis=0, concat_axis=0, tiled=True)

    other_half = swapped(my_ids[None], "px_0", 1)
    near = jnp.concatenate([my_ids[None], other_half])
    near = jnp.concatenate([near] + [swapped(near, ("py_1", CORE), bits) for bits in (1, 2, 3)])
    plane_ids = [near] + [swapped(near, "py_0", bits) for bits in (1, 2, 3)]
    place = lax.axis_index(PLANE).reshape(1, 1)
    outgoing = select(place, plane_ids, spread)
    outgoing, plane_ids, my_ids, peer_ids = lax.optimization_barrier(
        (outgoing, plane_ids, my_ids, near[2])
    )
    every_ids = jnp.concatenate(plane_ids)
    received = lax.all_to_all(outgoing, PLANE, split_axis=0, concat_axis=0, tiled=True)
    received = received.reshape(n_group, sizes[CORE], sizes["px_0"], SLOTS, n_z, part, BLK)
    received = pltpu.with_memory_space_constraint(received, pltpu.VMEM)
    for bit in (1, 2, 4):
        far = swapped(every_ids, "px_1", bit)
        every_ids = jnp.concatenate([every_ids, far])
    mate_ids = every_ids.reshape(n_z, sizes["py_0"], sizes["py_1"], 2, sizes["px_0"], SLOTS)
    mate_ids = mate_ids[:, :, :, 0].transpose(3, 2, 0, 1, 4)
    for dim, axis in enumerate(MATES):
        mate_ids = in_place_order(mate_ids, dim, axis)
    wanted = jnp.concatenate([my_ids, peer_ids])
    match = (wanted[:, None] == mate_ids.reshape(1, -1)).astype(F32)
    live = (my_ids < NBLK).astype(F32)
    column_live = jnp.repeat(live, BLK).reshape(1, WIDTH)
    column_live, match = lax.optimization_barrier((column_live, match))

    pixall = pixels * lax.axis_size(EVERY)
    tile_movie = pltpu.with_memory_space_constraint(movie.reshape(pixels, frames), pltpu.HBM)
    tile_foot = pltpu.with_memory_space_constraint(footprints.reshape(pixels, WIDTH), pltpu.HBM)
    current, colsq, cross, gram, inv = first_pass(
        my_ids[None], column_live, received, tile_movie, tile_foot
    )
    scale = live[:, None] / jnp.sqrt(totals_of(colsq, match) / pixall + 1e-06)
    current, colsq = second_pass(scale.reshape(1, WIDTH), current, cross, gram, inv)
    scale = live[:, None] / jnp.sqrt(totals_of(colsq, match) / pixall + 1e-06)
    return last_scaling(scale.reshape(1, WIDTH), current).reshape(rows, cols, WIDTH)


def solution(mesh):
    finer = Mesh(mesh.devices.reshape(4, 2, 2, 8, 2), EVERY)
    placed = (P(PY, PX, None), P(PY, PX), P(PY, PX, None), P(PY, PX, None))

    return jax.shard_map(
        per_device, mesh=finer, in_specs=placed, out_specs=P(PY, PX, None), check_vma=False
    )
```

```python
import jax
import jax.numpy as jnp
from jax import lax
from jax.experimental import pallas as pl
from jax.experimental.pallas import tpu as pltpu
from jax.sharding import Mesh
from jax.sharding import PartitionSpec as P


BLK = 128
SLOTS = 4
WIDTH = SLOTS * BLK
NBLK = 32
EVERY = ("py_0", "py_1", "px_0", "px_1", "px_2")
PY = ("py_0", "py_1")
PX = ("px_0", "px_1", "px_2")
COLUMN = ("py_0", "py_1", "px_1")
PLANE = ("py_0", "py_1", "px_2", "px_0")
MATES = ("px_0", "py_1", "px_1", "py_0")
CORE = "px_2"
F32 = jnp.float32
BF16 = jnp.bfloat16
ROW_TILE = 512
VMEM_BYTES = 24 << 20


def to_everyone(value, axes):
    copies = jnp.broadcast_to(value[None], (lax.axis_size(axes), *value.shape))
    return lax.all_to_all(copies, axes, split_axis=0, concat_axis=0, tiled=True)


def swapped(value, axis, bits):
    return lax.ppermute(value, axis, [(i, i ^ bits) for i in range(lax.axis_size(axis))])


def in_place_order(value, dim, axis):
    size = value.shape[dim]
    at = lax.axis_index(axis)
    bit = 1
    while bit < size:
        shape = (*value.shape[:dim], size // (2 * bit), 2, bit, *value.shape[dim + 1 :])
        flipped = jnp.flip(value.reshape(shape), dim + 1).reshape(value.shape)
        value = jnp.where((at & bit) != 0, flipped, value)
        bit *= 2
    return value


def stage_kernel(place_ref, *refs):
    *ids_refs, out_ref, sem = refs
    copies = [pltpu.make_async_copy(ids_ref, out_ref.at[i], sem) for i, ids_ref in enumerate(ids_refs)]
    out_ref[len(ids_refs), 0, 0] = place_ref[0, 0]
    for copy in copies:
        copy.start()
    for copy in copies:
        copy.wait()


def stage(place, ids_pieces):
    vmem = pl.BlockSpec(memory_space=pltpu.VMEM)
    smem = pl.BlockSpec(memory_space=pltpu.SMEM)
    n = len(ids_pieces)
    return pl.pallas_call(
        stage_kernel,
        out_shape=pltpu.SMEM((n + 1, *ids_pieces[0].shape), jnp.int32),
        in_specs=[smem] + [vmem] * n,
        out_specs=smem,
        scratch_shapes=[pltpu.SemaphoreType.DMA],
        compiler_params=pltpu.CompilerParams(vmem_limit_bytes=2 << 20),
        name="stage",
    )(place, *ids_pieces)


def select_kernel(ids_ref, rows_ref, out_hbm, sem):
    pieces, chunk, _ = ids_ref.shape
    pieces -= 1
    place = ids_ref[pieces, 0, 0]
    depth = rows_ref.shape[0] // (NBLK // SLOTS)
    for far in range(pieces):

        @pl.loop(0, chunk, unroll=True)
        def _(near):
            tile = (far * chunk + near) ^ place
            for slot in range(SLOTS):
                block = jnp.minimum(ids_ref[far, near, slot], NBLK - 1)
                group = pl.multiple_of((block // SLOTS) * depth, depth)
                lane = pl.multiple_of((block % SLOTS) * BLK, BLK)
                pltpu.make_async_copy(
                    rows_ref.at[pl.ds(group, depth), :, pl.ds(lane, BLK)],
                    out_hbm.at[tile, slot],
                    sem,
                ).start()

    pltpu.make_async_copy(out_hbm, out_hbm, sem).wait()


def select(staged, rows):
    depth = rows.shape[0] // (NBLK // SLOTS)
    tiles = (staged.shape[0] - 1) * staged.shape[1]
    return pl.pallas_call(
        select_kernel,
        out_shape=jax.ShapeDtypeStruct((tiles, SLOTS, depth, rows.shape[1], BLK), rows.dtype),
        in_specs=[pl.BlockSpec(memory_space=pltpu.SMEM), pl.BlockSpec(memory_space=pltpu.VMEM)],
        out_specs=pl.BlockSpec(memory_space=pltpu.HBM),
        scratch_shapes=[pltpu.SemaphoreType.DMA],
        compiler_params=pltpu.CompilerParams(vmem_limit_bytes=2 << 20),
        cost_estimate=pl.CostEstimate(flops=1 << 20, bytes_accessed=1 << 22, transcendentals=0),
        name="select",
    )(staged, rows)


def sweep(base, a_ref, hi_ref, lo_ref, cross_ref, gram_ref, inv_ref, colsq_ref):
    pixels = a_ref.shape[0]
    for slot in range(SLOTS):
        c = slice(slot * BLK, (slot + 1) * BLK)
        weights = gram_ref[slot]
        total = jnp.zeros((1, BLK), F32)
        for low in range(0, pixels, ROW_TILE):
            r = slice(low, low + ROW_TILE)
            both = jnp.dot(hi_ref[r, :], weights, preferred_element_type=F32)
            both += jnp.dot(lo_ref[r, :], weights, preferred_element_type=F32)
            resid = cross_ref[r, c] - (both[:, :BLK] + both[:, BLK:])
            fresh = jnp.maximum(base(r, c) + resid * inv_ref[:, c], 0.0)
            a_ref[r, c] = fresh
            if slot < SLOTS - 1:
                high = fresh.astype(BF16)
                hi_ref[r, c] = high
                lo_ref[r, c] = (fresh - high.astype(F32)).astype(BF16)
            total += jnp.sum(fresh * fresh, axis=0, keepdims=True)
        colsq_ref[slot : slot + 1, :] = total


def put_parts(value, r, hi_ref, lo_ref):
    high = value.astype(BF16)
    hi_ref[r, :] = high
    lo_ref[r, :] = (value - high.astype(F32)).astype(BF16)


def first_kernel(
    ids_ref, live_ref, recv_ref, movie_hbm, foot_hbm,
    a_ref, colsq_ref, cross_ref, gram_ref, inv_ref,
    movie_ref, foot_ref, picked_ref, square_ref, hi_ref, lo_ref, sems,
):
    pixels = movie_ref.shape[0]
    tiles = [slice(low, low + ROW_TILE) for low in range(0, pixels, ROW_TILE)]
    movies = [
        pltpu.make_async_copy(movie_hbm.at[r, :], movie_ref.at[r, :], sems.at[i])
        for i, r in enumerate(tiles)
    ]
    foots = [
        pltpu.make_async_copy(foot_hbm.at[r, :], foot_ref.at[r, :], sems.at[len(tiles) + i])
        for i, r in enumerate(tiles)
    ]
    for copy in movies + foots:
        copy.start()
    groups, cores, halves, _, depth, part, _ = recv_ref.shape
    size = groups * part
    base = 0
    for half in range(halves):
        for z in range(depth):
            for core in range(cores):
                for slot in range(SLOTS):
                    piece = recv_ref[:, core, half, slot, z].astype(F32).reshape(size, BLK)
                    picked_ref[base : base + size, slot * BLK : (slot + 1) * BLK] = piece.astype(BF16)
                base += size
    for slot in range(SLOTS):

        @pl.when(ids_ref[0, slot] >= NBLK)
        def _():
            picked_ref[:, slot * BLK : (slot + 1) * BLK] = jnp.zeros((picked_ref.shape[0], BLK), BF16)

    picked = picked_ref[...]
    square_ref[...] = lax.dot_general(
        picked, picked, (((0,), (0,)), ((), ())), preferred_element_type=F32
    )
    eye = lax.broadcasted_iota(jnp.int32, (BLK, BLK), 0) == lax.broadcasted_iota(
        jnp.int32, (BLK, BLK), 1
    )
    for slot in range(SLOTS):
        c = slice(slot * BLK, (slot + 1) * BLK)
        columns = square_ref[:, c]
        high = columns.astype(BF16)
        gram_ref[slot, :, :BLK] = high
        gram_ref[slot, :, BLK:] = (columns - high.astype(F32)).astype(BF16)
        diagonal = jnp.sum(jnp.where(eye, square_ref[c, c], 0.0), axis=0, keepdims=True)
        inv_ref[:, c] = 1.0 / (diagonal + 1e-06 + (1.0 - live_ref[:, c]))
    for r, copy in zip(tiles, movies):
        copy.wait()
        cross_ref[r, :] = jnp.dot(movie_ref[r, :], picked, preferred_element_type=F32)
    for r, copy in zip(tiles, foots):
        copy.wait()
        put_parts(foot_ref[r, :] * live_ref[...], r, hi_ref, lo_ref)
    sweep(
        lambda r, c: foot_ref[r, c] * live_ref[:, c],
        a_ref, hi_ref, lo_ref, cross_ref, gram_ref, inv_ref, colsq_ref,
    )


def second_kernel(
    scale_ref, old_ref, cross_ref, gram_ref, inv_ref, a_ref, colsq_ref, hi_ref, lo_ref
):
    for low in range(0, old_ref.shape[0], ROW_TILE):
        r = slice(low, low + ROW_TILE)
        put_parts(old_ref[r, :] * scale_ref[...], r, hi_ref, lo_ref)
    sweep(
        lambda r, c: old_ref[r, c] * scale_ref[:, c],
        a_ref, hi_ref, lo_ref, cross_ref, gram_ref, inv_ref, colsq_ref,
    )


def last_kernel(scale_ref, a_ref, out_hbm, buffer_ref, sems):
    step = buffer_ref.shape[0] // sems.shape[0]
    copies = []
    for i in range(sems.shape[0]):
        r = slice(i * step, (i + 1) * step)
        buffer_ref[r, :] = a_ref[r, :] * scale_ref[...]
        copy = pltpu.make_async_copy(buffer_ref.at[r, :], out_hbm.at[r, :], sems.at[i])
        copy.start()
        copies.append(copy)
    for copy in copies:
        copy.wait()


VMEM_SPEC = pl.BlockSpec(memory_space=pltpu.VMEM)
HBM_SPEC = pl.BlockSpec(memory_space=pltpu.HBM)
SMEM_SPEC = pl.BlockSpec(memory_space=pltpu.SMEM)


def first_pass(ids, live, received, tile_movie, tile_foot):
    pixels, frames = tile_movie.shape
    return pl.pallas_call(
        first_kernel,
        out_shape=(
            pltpu.VMEM((pixels, WIDTH), F32),
            pltpu.VMEM((SLOTS, BLK), F32),
            pltpu.VMEM((pixels, WIDTH), F32),
            pltpu.VMEM((SLOTS, WIDTH, 2 * BLK), BF16),
            pltpu.VMEM((1, WIDTH), F32),
        ),
        in_specs=[SMEM_SPEC] + [VMEM_SPEC] * 2 + [HBM_SPEC] * 2,
        out_specs=(VMEM_SPEC,) * 5,
        scratch_shapes=[
            pltpu.VMEM((pixels, frames), BF16),
            pltpu.VMEM((pixels, WIDTH), F32),
            pltpu.VMEM((frames, WIDTH), BF16),
            pltpu.VMEM((WIDTH, WIDTH), F32),
            pltpu.VMEM((pixels, WIDTH), BF16),
            pltpu.VMEM((pixels, WIDTH), BF16),
            pltpu.SemaphoreType.DMA((2 * pixels // ROW_TILE,)),
        ],
        compiler_params=pltpu.CompilerParams(vmem_limit_bytes=2 * VMEM_BYTES),
        cost_estimate=pl.CostEstimate(flops=7 << 30, bytes_accessed=12 << 20, transcendentals=0),
        name="first_pass",
    )(ids, live, received, tile_movie, tile_foot)


def second_pass(scale, a, cross, gram, inv):
    pixels = a.shape[0]
    return pl.pallas_call(
        second_kernel,
        out_shape=(pltpu.VMEM((pixels, WIDTH), F32), pltpu.VMEM((SLOTS, BLK), F32)),
        in_specs=[VMEM_SPEC] * 5,
        out_specs=(VMEM_SPEC,) * 2,
        scratch_shapes=[pltpu.VMEM((pixels, WIDTH), BF16), pltpu.VMEM((pixels, WIDTH), BF16)],
        compiler_params=pltpu.CompilerParams(vmem_limit_bytes=VMEM_BYTES),
        cost_estimate=pl.CostEstimate(flops=4 << 30, bytes_accessed=8 << 20, transcendentals=0),
        name="second_pass",
    )(scale, a, cross, gram, inv)


def last_scaling(scale, a):
    return pl.pallas_call(
        last_kernel,
        out_shape=jax.ShapeDtypeStruct(a.shape, F32),
        in_specs=[VMEM_SPEC] * 2,
        out_specs=HBM_SPEC,
        scratch_shapes=[pltpu.VMEM(a.shape, F32), pltpu.SemaphoreType.DMA((8,))],
        compiler_params=pltpu.CompilerParams(vmem_limit_bytes=4 << 20),
        name="last_scaling",
    )(scale, a)


def totals_of(colsq, match):
    seen = to_everyone(colsq, MATES).reshape(-1, BLK)
    sums = jnp.dot(match, seen, precision=lax.Precision.HIGHEST)
    return sums[:SLOTS] + swapped(sums[SLOTS:], CORE, 1)


def per_device(movie, traces, footprints, block_ids):
    rows, cols, frames = movie.shape
    pixels = rows * cols
    n_group = lax.axis_size(PY)
    n_z = lax.axis_size("px_1")
    sizes = {axis: lax.axis_size(axis) for axis in EVERY}
    part = traces.shape[1] // n_group
    my_ids = block_ids.reshape(SLOTS)

    pieces = traces.T.reshape(n_group, 1, part, traces.shape[0])
    pieces = jnp.broadcast_to(pieces, (n_group, n_z, part, traces.shape[0]))
    pieces = pieces.reshape(n_group * n_z, part, traces.shape[0])
    pieces = pltpu.with_memory_space_constraint(pieces, pltpu.VMEM)
    spread = lax.all_to_all(pieces, COLUMN, split_axis=0, concat_axis=0, tiled=True)

    other_half = swapped(my_ids[None], "px_0", 1)
    near = jnp.concatenate([my_ids[None], other_half])
    near = jnp.concatenate([near] + [swapped(near, ("py_1", CORE), bits) for bits in (1, 2, 3)])
    plane_ids = [near] + [swapped(near, "py_0", bits) for bits in (1, 2, 3)]
    place = lax.axis_index(PLANE).reshape(1, 1)
    outgoing = select(stage(place, plane_ids), spread)
    outgoing, plane_ids, my_ids, peer_ids = lax.optimization_barrier(
        (outgoing, plane_ids, my_ids, near[2])
    )
    every_ids = jnp.concatenate(plane_ids)
    received = lax.all_to_all(outgoing, PLANE, split_axis=0, concat_axis=0, tiled=True)
    received = received.reshape(n_group, sizes[CORE], sizes["px_0"], SLOTS, n_z, part, BLK)
    received = pltpu.with_memory_space_constraint(received, pltpu.VMEM)
    for bit in (1, 2, 4):
        far = swapped(every_ids, "px_1", bit)
        every_ids = jnp.concatenate([every_ids, far])
    mate_ids = every_ids.reshape(n_z, sizes["py_0"], sizes["py_1"], 2, sizes["px_0"], SLOTS)
    mate_ids = mate_ids[:, :, :, 0].transpose(3, 2, 0, 1, 4)
    for dim, axis in enumerate(MATES):
        mate_ids = in_place_order(mate_ids, dim, axis)
    wanted = jnp.concatenate([my_ids, peer_ids])
    match = (wanted[:, None] == mate_ids.reshape(1, -1)).astype(F32)
    live = (my_ids < NBLK).astype(F32)
    column_live = jnp.repeat(live, BLK).reshape(1, WIDTH)
    column_live, match = lax.optimization_barrier((column_live, match))

    pixall = pixels * lax.axis_size(EVERY)
    tile_movie = pltpu.with_memory_space_constraint(movie.reshape(pixels, frames), pltpu.HBM)
    tile_foot = pltpu.with_memory_space_constraint(footprints.reshape(pixels, WIDTH), pltpu.HBM)
    current, colsq, cross, gram, inv = first_pass(
        my_ids[None], column_live, received, tile_movie, tile_foot
    )
    scale = live[:, None] / jnp.sqrt(totals_of(colsq, match) / pixall + 1e-06)
    current, colsq = second_pass(scale.reshape(1, WIDTH), current, cross, gram, inv)
    scale = live[:, None] / jnp.sqrt(totals_of(colsq, match) / pixall + 1e-06)
    return last_scaling(scale.reshape(1, WIDTH), current).reshape(rows, cols, WIDTH)


def solution(mesh):
    finer = Mesh(mesh.devices.reshape(4, 2, 2, 8, 2), EVERY)
    placed = (P(PY, PX, None), P(PY, PX), P(PY, PX, None), P(PY, PX, None))

    return jax.shard_map(
        per_device, mesh=finer, in_specs=placed, out_specs=P(PY, PX, None), check_vma=False
    )
```

```python
import jax
import jax.numpy as jnp
from jax import lax
from jax.experimental import pallas as pl
from jax.experimental.pallas import tpu as pltpu
from jax.sharding import Mesh
from jax.sharding import PartitionSpec as P


BLK = 128
SLOTS = 4
WIDTH = SLOTS * BLK
NBLK = 32
EVERY = ("py_0", "py_1", "px_0", "px_1", "px_2")
PY = ("py_0", "py_1")
PX = ("px_0", "px_1", "px_2")
COLUMN = ("py_0", "py_1", "px_1")
PLANE = ("py_0", "py_1", "px_2", "px_0")
MATES = ("px_0", "py_1", "px_1", "py_0")
CORE = "px_2"
F32 = jnp.float32
BF16 = jnp.bfloat16
ROW_TILE = 512
VMEM_BYTES = 24 << 20


def to_everyone(value, axes):
    copies = jnp.broadcast_to(value[None], (lax.axis_size(axes), *value.shape))
    return lax.all_to_all(copies, axes, split_axis=0, concat_axis=0, tiled=True)


def swapped(value, axis, bits):
    return lax.ppermute(value, axis, [(i, i ^ bits) for i in range(lax.axis_size(axis))])


def in_place_order(value, dim, axis):
    size = value.shape[dim]
    at = lax.axis_index(axis)
    bit = 1
    while bit < size:
        shape = (*value.shape[:dim], size // (2 * bit), 2, bit, *value.shape[dim + 1 :])
        flipped = jnp.flip(value.reshape(shape), dim + 1).reshape(value.shape)
        value = jnp.where((at & bit) != 0, flipped, value)
        bit *= 2
    return value


def stage_kernel(place_ref, *refs):
    *ids_refs, out_ref, sem = refs
    copies = [pltpu.make_async_copy(ids_ref, out_ref.at[i], sem) for i, ids_ref in enumerate(ids_refs)]
    out_ref[len(ids_refs), 0, 0] = place_ref[0, 0]
    for copy in copies:
        copy.start()
    for copy in copies:
        copy.wait()


def stage(place, ids_pieces):
    vmem = pl.BlockSpec(memory_space=pltpu.VMEM)
    smem = pl.BlockSpec(memory_space=pltpu.SMEM)
    n = len(ids_pieces)
    return pl.pallas_call(
        stage_kernel,
        out_shape=pltpu.SMEM((n + 1, *ids_pieces[0].shape), jnp.int32),
        in_specs=[smem] + [vmem] * n,
        out_specs=smem,
        scratch_shapes=[pltpu.SemaphoreType.DMA],
        compiler_params=pltpu.CompilerParams(vmem_limit_bytes=2 << 20),
        name="stage",
    )(place, *ids_pieces)


def select_kernel(ids_ref, rows_ref, out_hbm, sem):
    pieces, chunk, _ = ids_ref.shape
    pieces -= 1
    place = ids_ref[pieces, 0, 0]
    depth = rows_ref.shape[0] // (NBLK // SLOTS)
    for far in range(pieces):

        @pl.loop(0, chunk, unroll=True)
        def _(near):
            tile = (far * chunk + near) ^ place
            for slot in range(SLOTS):
                block = jnp.minimum(ids_ref[far, near, slot], NBLK - 1)
                group = pl.multiple_of((block // SLOTS) * depth, depth)
                lane = pl.multiple_of((block % SLOTS) * BLK, BLK)
                pltpu.make_async_copy(
                    rows_ref.at[pl.ds(group, depth), :, pl.ds(lane, BLK)],
                    out_hbm.at[tile, slot],
                    sem,
                ).start()

    pltpu.make_async_copy(out_hbm, out_hbm, sem).wait()


def select(staged, rows):
    depth = rows.shape[0] // (NBLK // SLOTS)
    tiles = (staged.shape[0] - 1) * staged.shape[1]
    return pl.pallas_call(
        select_kernel,
        out_shape=jax.ShapeDtypeStruct((tiles, SLOTS, depth, rows.shape[1], BLK), rows.dtype),
        in_specs=[pl.BlockSpec(memory_space=pltpu.SMEM), pl.BlockSpec(memory_space=pltpu.VMEM)],
        out_specs=pl.BlockSpec(memory_space=pltpu.HBM),
        scratch_shapes=[pltpu.SemaphoreType.DMA],
        compiler_params=pltpu.CompilerParams(vmem_limit_bytes=2 << 20),
        cost_estimate=pl.CostEstimate(flops=1 << 20, bytes_accessed=1 << 22, transcendentals=0),
        name="select",
    )(staged, rows)


def sweep(base, a_ref, hi_ref, lo_ref, cross_ref, gram_ref, inv_ref, colsq_ref):
    pixels = a_ref.shape[0]
    for slot in range(SLOTS):
        c = slice(slot * BLK, (slot + 1) * BLK)
        weights = gram_ref[slot]
        total = jnp.zeros((1, BLK), F32)
        for low in range(0, pixels, ROW_TILE):
            r = slice(low, low + ROW_TILE)
            both = jnp.dot(hi_ref[r, :], weights, preferred_element_type=F32)
            both += jnp.dot(lo_ref[r, :], weights, preferred_element_type=F32)
            resid = cross_ref[r, c] - (both[:, :BLK] + both[:, BLK:])
            fresh = jnp.maximum(base(r, c) + resid * inv_ref[:, c], 0.0)
            a_ref[r, c] = fresh
            if slot < SLOTS - 1:
                high = fresh.astype(BF16)
                hi_ref[r, c] = high
                lo_ref[r, c] = (fresh - high.astype(F32)).astype(BF16)
            total += jnp.sum(fresh * fresh, axis=0, keepdims=True)
        colsq_ref[slot : slot + 1, :] = total


def put_parts(value, r, hi_ref, lo_ref):
    high = value.astype(BF16)
    hi_ref[r, :] = high
    lo_ref[r, :] = (value - high.astype(F32)).astype(BF16)


def first_kernel(
    ids_ref, live_ref, recv_ref, movie_hbm, foot_hbm,
    a_ref, colsq_ref, cross_ref, gram_ref, inv_ref,
    movie_ref, foot_ref, picked_ref, square_ref, hi_ref, lo_ref, sems,
):
    pixels = movie_ref.shape[0]
    tiles = [slice(low, low + ROW_TILE) for low in range(0, pixels, ROW_TILE)]
    movies = [
        pltpu.make_async_copy(movie_hbm.at[r, :], movie_ref.at[r, :], sems.at[i])
        for i, r in enumerate(tiles)
    ]
    foots = [
        pltpu.make_async_copy(foot_hbm.at[r, :], foot_ref.at[r, :], sems.at[len(tiles) + i])
        for i, r in enumerate(tiles)
    ]
    for copy in movies + foots:
        copy.start()
    groups, cores, halves, _, depth, part, _ = recv_ref.shape
    size = groups * part
    base = 0
    for half in range(halves):
        for z in range(depth):
            for core in range(cores):
                for slot in range(SLOTS):
                    piece = recv_ref[:, core, half, slot, z].astype(F32).reshape(size, BLK)
                    picked_ref[base : base + size, slot * BLK : (slot + 1) * BLK] = piece.astype(BF16)
                base += size
    for slot in range(SLOTS):

        @pl.when(ids_ref[0, 0, slot] >= NBLK)
        def _():
            picked_ref[:, slot * BLK : (slot + 1) * BLK] = jnp.zeros((picked_ref.shape[0], BLK), BF16)

    picked = picked_ref[...]
    square_ref[...] = lax.dot_general(
        picked, picked, (((0,), (0,)), ((), ())), preferred_element_type=F32
    )
    eye = lax.broadcasted_iota(jnp.int32, (BLK, BLK), 0) == lax.broadcasted_iota(
        jnp.int32, (BLK, BLK), 1
    )
    for slot in range(SLOTS):
        c = slice(slot * BLK, (slot + 1) * BLK)
        columns = square_ref[:, c]
        high = columns.astype(BF16)
        gram_ref[slot, :, :BLK] = high
        gram_ref[slot, :, BLK:] = (columns - high.astype(F32)).astype(BF16)
        diagonal = jnp.sum(jnp.where(eye, square_ref[c, c], 0.0), axis=0, keepdims=True)
        inv_ref[:, c] = 1.0 / (diagonal + 1e-06 + (1.0 - live_ref[:, c]))
    for r, copy in zip(tiles, movies):
        copy.wait()
        cross_ref[r, :] = jnp.dot(movie_ref[r, :], picked, preferred_element_type=F32)
    for r, copy in zip(tiles, foots):
        copy.wait()
        put_parts(foot_ref[r, :] * live_ref[...], r, hi_ref, lo_ref)
    sweep(
        lambda r, c: foot_ref[r, c] * live_ref[:, c],
        a_ref, hi_ref, lo_ref, cross_ref, gram_ref, inv_ref, colsq_ref,
    )


def second_kernel(
    scale_ref, old_ref, cross_ref, gram_ref, inv_ref, a_ref, colsq_ref, hi_ref, lo_ref
):
    for low in range(0, old_ref.shape[0], ROW_TILE):
        r = slice(low, low + ROW_TILE)
        put_parts(old_ref[r, :] * scale_ref[...], r, hi_ref, lo_ref)
    sweep(
        lambda r, c: old_ref[r, c] * scale_ref[:, c],
        a_ref, hi_ref, lo_ref, cross_ref, gram_ref, inv_ref, colsq_ref,
    )


def last_kernel(scale_ref, a_ref, out_hbm, buffer_ref, sems):
    step = buffer_ref.shape[0] // sems.shape[0]
    copies = []
    for i in range(sems.shape[0]):
        r = slice(i * step, (i + 1) * step)
        buffer_ref[r, :] = a_ref[r, :] * scale_ref[...]
        copy = pltpu.make_async_copy(buffer_ref.at[r, :], out_hbm.at[r, :], sems.at[i])
        copy.start()
        copies.append(copy)
    for copy in copies:
        copy.wait()


VMEM_SPEC = pl.BlockSpec(memory_space=pltpu.VMEM)
HBM_SPEC = pl.BlockSpec(memory_space=pltpu.HBM)
SMEM_SPEC = pl.BlockSpec(memory_space=pltpu.SMEM)


def first_pass(ids, live, received, tile_movie, tile_foot):
    pixels, frames = tile_movie.shape
    return pl.pallas_call(
        first_kernel,
        out_shape=(
            pltpu.VMEM((pixels, WIDTH), F32),
            pltpu.VMEM((SLOTS, BLK), F32),
            pltpu.VMEM((pixels, WIDTH), F32),
            pltpu.VMEM((SLOTS, WIDTH, 2 * BLK), BF16),
            pltpu.VMEM((1, WIDTH), F32),
        ),
        in_specs=[SMEM_SPEC] + [VMEM_SPEC] * 2 + [HBM_SPEC] * 2,
        out_specs=(VMEM_SPEC,) * 5,
        scratch_shapes=[
            pltpu.VMEM((pixels, frames), BF16),
            pltpu.VMEM((pixels, WIDTH), F32),
            pltpu.VMEM((frames, WIDTH), BF16),
            pltpu.VMEM((WIDTH, WIDTH), F32),
            pltpu.VMEM((pixels, WIDTH), BF16),
            pltpu.VMEM((pixels, WIDTH), BF16),
            pltpu.SemaphoreType.DMA((2 * pixels // ROW_TILE,)),
        ],
        compiler_params=pltpu.CompilerParams(vmem_limit_bytes=2 * VMEM_BYTES),
        cost_estimate=pl.CostEstimate(flops=7 << 30, bytes_accessed=12 << 20, transcendentals=0),
        name="first_pass",
    )(ids, live, received, tile_movie, tile_foot)


def second_pass(scale, a, cross, gram, inv):
    pixels = a.shape[0]
    return pl.pallas_call(
        second_kernel,
        out_shape=(pltpu.VMEM((pixels, WIDTH), F32), pltpu.VMEM((SLOTS, BLK), F32)),
        in_specs=[VMEM_SPEC] * 5,
        out_specs=(VMEM_SPEC,) * 2,
        scratch_shapes=[pltpu.VMEM((pixels, WIDTH), BF16), pltpu.VMEM((pixels, WIDTH), BF16)],
        compiler_params=pltpu.CompilerParams(vmem_limit_bytes=VMEM_BYTES),
        cost_estimate=pl.CostEstimate(flops=4 << 30, bytes_accessed=8 << 20, transcendentals=0),
        name="second_pass",
    )(scale, a, cross, gram, inv)


def last_scaling(scale, a):
    return pl.pallas_call(
        last_kernel,
        out_shape=jax.ShapeDtypeStruct(a.shape, F32),
        in_specs=[VMEM_SPEC] * 2,
        out_specs=HBM_SPEC,
        scratch_shapes=[pltpu.VMEM(a.shape, F32), pltpu.SemaphoreType.DMA((8,))],
        compiler_params=pltpu.CompilerParams(vmem_limit_bytes=4 << 20),
        name="last_scaling",
    )(scale, a)


def totals_of(colsq, match):
    seen = to_everyone(colsq, MATES).reshape(-1, BLK)
    sums = jnp.dot(match, seen, precision=lax.Precision.HIGHEST)
    return sums[:SLOTS] + swapped(sums[SLOTS:], CORE, 1)


def per_device(movie, traces, footprints, block_ids):
    rows, cols, frames = movie.shape
    pixels = rows * cols
    n_group = lax.axis_size(PY)
    n_z = lax.axis_size("px_1")
    sizes = {axis: lax.axis_size(axis) for axis in EVERY}
    part = traces.shape[1] // n_group
    my_ids = block_ids.reshape(SLOTS)

    pieces = traces.T.reshape(n_group, 1, part, traces.shape[0])
    pieces = jnp.broadcast_to(pieces, (n_group, n_z, part, traces.shape[0]))
    pieces = pieces.reshape(n_group * n_z, part, traces.shape[0])
    pieces = pltpu.with_memory_space_constraint(pieces, pltpu.VMEM)
    spread = lax.all_to_all(pieces, COLUMN, split_axis=0, concat_axis=0, tiled=True)

    other_half = swapped(my_ids[None], "px_0", 1)
    near = jnp.concatenate([my_ids[None], other_half])
    near = jnp.concatenate([near] + [swapped(near, ("py_1", CORE), bits) for bits in (1, 2, 3)])
    plane_ids = [near] + [swapped(near, "py_0", bits) for bits in (1, 2, 3)]
    place = lax.axis_index(PLANE).reshape(1, 1)
    staged = stage(place, plane_ids)
    outgoing = select(staged, spread)
    outgoing, plane_ids, my_ids, peer_ids = lax.optimization_barrier(
        (outgoing, plane_ids, my_ids, near[2])
    )
    every_ids = jnp.concatenate(plane_ids)
    received = lax.all_to_all(outgoing, PLANE, split_axis=0, concat_axis=0, tiled=True)
    received = received.reshape(n_group, sizes[CORE], sizes["px_0"], SLOTS, n_z, part, BLK)
    received = pltpu.with_memory_space_constraint(received, pltpu.VMEM)
    for bit in (1, 2, 4):
        far = swapped(every_ids, "px_1", bit)
        every_ids = jnp.concatenate([every_ids, far])
    mate_ids = every_ids.reshape(n_z, sizes["py_0"], sizes["py_1"], 2, sizes["px_0"], SLOTS)
    mate_ids = mate_ids[:, :, :, 0].transpose(3, 2, 0, 1, 4)
    for dim, axis in enumerate(MATES):
        mate_ids = in_place_order(mate_ids, dim, axis)
    wanted = jnp.concatenate([my_ids, peer_ids])
    match = (wanted[:, None] == mate_ids.reshape(1, -1)).astype(F32)
    live = (my_ids < NBLK).astype(F32)
    column_live = jnp.repeat(live, BLK).reshape(1, WIDTH)
    column_live, match = lax.optimization_barrier((column_live, match))

    pixall = pixels * lax.axis_size(EVERY)
    tile_movie = pltpu.with_memory_space_constraint(movie.reshape(pixels, frames), pltpu.HBM)
    tile_foot = pltpu.with_memory_space_constraint(footprints.reshape(pixels, WIDTH), pltpu.HBM)
    current, colsq, cross, gram, inv = first_pass(
        staged, column_live, received, tile_movie, tile_foot
    )
    scale = live[:, None] / jnp.sqrt(totals_of(colsq, match) / pixall + 1e-06)
    current, colsq = second_pass(scale.reshape(1, WIDTH), current, cross, gram, inv)
    scale = live[:, None] / jnp.sqrt(totals_of(colsq, match) / pixall + 1e-06)
    return last_scaling(scale.reshape(1, WIDTH), current).reshape(rows, cols, WIDTH)


def solution(mesh):
    finer = Mesh(mesh.devices.reshape(4, 2, 2, 8, 2), EVERY)
    placed = (P(PY, PX, None), P(PY, PX), P(PY, PX, None), P(PY, PX, None))

    return jax.shard_map(
        per_device, mesh=finer, in_specs=placed, out_specs=P(PY, PX, None), check_vma=False
    )
```
